32 devices in a mesh: tm: 8 (over y, x, core), gy: 4 (over z).
Axes of the slice: x: 2, y: 2, z: 4, core: 2. Of those that a mesh axis runs over, the one named last changes fastest.
Arguments:
- initial_state: float32 [3, 64, 1024], P(None, 'gy'), may hold values from -4 to 4
- guessed_ends: float32 [8, 3, 64, 1024], P('tm', None, 'gy'), may hold values from -4 to 4
- velocity: float32 [8, 2, 64, 1024], P('tm', None, 'gy'), may hold values from -1 to 1
Outputs:
- corrected: float32 [8, 3, 64, 1024], P('tm', None, 'gy')
- relaxed: float32 [8, 3, 64, 1024], P('tm', None, 'gy')
The draws below stay inside these ranges and needn't reach their ends.
All inputs are finite; a program needn't handle non-finite values.
Results may differ from the reference program's by a relative error of at most 0.00002.
Values sent between devices are 32-bit elements; how exact they have to be, the bound alone decides.
A program may use at most 64 MiB of HBM per device.

```python
import jax
import jax.numpy as jnp

NX = 1024
FINE = 4
GROUP = 4
NY = 64
INTERVALS = 8
N_TM = 8


def shard_levels(key, dims, shards, smallest, top_value):
    loudness, own = 1.0, jax.random.fold_in(key, 6)
    for position, shards_of in shards:
        heights = jnp.exp(jax.random.uniform(jax.random.fold_in(own, position), (shards_of,), jnp.float32, smallest / len(shards), top_value / len(shards)))
        loudness = loudness * jnp.repeat(heights, dims[position] // shards_of).reshape([-1 if axis == position else 1 for axis in range(len(dims))])
    return loudness


def normal_values(own_key, dims, scale, bound, split=(), held_as=jnp.bfloat16):
    loudness = shard_levels(own_key, dims, split, -0.22, 0.18) if split else 1.0
    entries = jax.random.normal(own_key, dims, jnp.float32) * scale * loudness
    return jnp.minimum(jnp.maximum(entries, -bound), bound).astype(held_as)


def setup_inputs(seed: int = 0) -> dict:
    keys = jax.random.split(jax.random.key(seed), 4)
    initial_state = normal_values(keys[0], (3, NY, NX), 1.0, 4.0, ((1, 4),), jnp.float32)
    guessed_ends = normal_values(keys[1], (INTERVALS, 3, NY, NX), 1.0, 4.0, ((0, 8), (2, 4)), jnp.float32)
    velocity = jnp.clip(jax.random.uniform(keys[2], (INTERVALS, 2, NY, NX), jnp.float32, -1.0, 1.0) * shard_levels(keys[2], (INTERVALS, 2, NY, NX), ((0, 8), (2, 4)), -0.4, 0.0), -1.0, 1.0)
    return {"initial_state": initial_state, "guessed_ends": guessed_ends, "velocity": velocity}


diffusion = (0.05, 0.15, 0.4)
kappa_coupling = 0.1
time_step = 0.0125


def advance(extended, velocity, factor):
    center = extended[:, 1:-1]
    northern = extended[:, 2:]
    southern = extended[:, :-2]
    eastern = jnp.roll(center, -1, axis=2)
    western = jnp.roll(center, 1, axis=2)
    speed_across = velocity[0] + kappa_coupling * center[0]
    speed_along = velocity[1] + kappa_coupling * center[1]
    transport = jnp.maximum(speed_across, 0.0) * (center - western) + jnp.minimum(speed_across, 0.0) * (eastern - center)
    transport = transport + jnp.maximum(speed_along, 0.0) * (center - southern) + jnp.minimum(speed_along, 0.0) * (northern - center)
    spread = northern + southern + eastern + western - 4.0 * center
    viscous = jnp.array(diffusion, jnp.float32)[:, None, None]
    return center + factor * (viscous * spread - transport)


def one_step(state, velocity, factor):
    extended = jnp.pad(state, ((0, 0), (1, 1), (0, 0)))
    return advance(extended, velocity, factor)


def interval(state, velocity):
    for section in range(FINE):
        state = one_step(state, velocity, time_step)
    return state


def reference(initial_state, guessed_ends, velocity):
    level_one = FINE * time_step
    coarsest = FINE * GROUP * time_step
    stepper = jax.vmap(one_step, in_axes=(0, 0, None))
    begins = jnp.concatenate([initial_state[None], guessed_ends[:-1]], axis=0)
    fine_ends = jax.vmap(interval)(begins, velocity)
    coarse_begin = stepper(begins, velocity, level_one)
    sources = fine_ends - coarse_begin
    current = coarse_begin[0::GROUP] + sources[0::GROUP]
    for k in range(1, GROUP):
        current = stepper(current, velocity[k::GROUP], level_one) + sources[k::GROUP]
    forcing = current - stepper(begins[0::GROUP], velocity[GROUP - 1::GROUP], coarsest)
    chain = []
    state = initial_state
    for j in range(N_TM // GROUP):
        state = one_step(state, velocity[GROUP * j + GROUP - 1], coarsest) + forcing[j]
        chain.append(state)
    settled = jnp.stack(chain)
    current = jnp.concatenate([initial_state[None], settled[:-1]], axis=0)
    columns = []
    for k in range(GROUP - 1):
        current = stepper(current, velocity[k::GROUP], level_one) + sources[k::GROUP]
        columns.append(current)
    columns.append(settled)
    corrected = jnp.stack(columns, axis=1).reshape(guessed_ends.shape)
    final_begins = jnp.concatenate([initial_state[None], corrected[:-1]], axis=0)
    relaxed = jax.vmap(interval)(final_begins, velocity)
    return corrected, relaxed
```

```python
import functools

import jax
import jax.numpy as jnp
from jax import lax
from jax.experimental import pallas as pl
from jax.experimental.pallas import tpu as pltpu
from jax.sharding import PartitionSpec as P

FINE = 4
GROUP = 4
LANES = 128
BLOCK = 4

diffusion = (0.05, 0.15, 0.4)
kappa_coupling = 0.1
time_step = 0.0125

VLO, VHI, BC, BLO, BHI, AC, ALO, AHI, LC, LLO, LHI, DC, DLO, DHI, SC, SLO, SHI, KINDS = range(18)
SENDS = 24


def shifted(x, by):
    sub, lanes = x.shape[-2:]
    lane = lax.broadcasted_iota(jnp.int32, (1, sub, lanes), 2)
    if by == 1:
        turned = pltpu.roll(x, lanes - 1, 2)
        return jnp.where(lane == lanes - 1, pltpu.roll(turned, sub - 1, 1), turned)
    turned = pltpu.roll(x, 1, 2)
    return jnp.where(lane == 0, pltpu.roll(turned, 1, 1), turned)


def step_rows(src, first, vel, vfirst, count, factor):
    vx, vy = vel[vfirst : vfirst + count, 0], vel[vfirst : vfirst + count, 1]
    u0 = src[first : first + count, 0]
    u1 = src[first : first + count, 1]
    ax = vx + kappa_coupling * u0
    ay = vy + kappa_coupling * u1
    axp, axn = jnp.maximum(ax, 0.0), jnp.minimum(ax, 0.0)
    ayp, ayn = jnp.maximum(ay, 0.0), jnp.minimum(ay, 0.0)
    out = []
    for c in range(3):
        u = (u0, u1)[c] if c < 2 else src[first : first + count, 2]
        n = src[first + 1 : first + 1 + count, c]
        s = src[first - 1 : first - 1 + count, c]
        e, w = shifted(u, 1), shifted(u, -1)
        adv = axp * (u - w) + axn * (e - u)
        adv = adv + ayp * (u - s) + ayn * (n - u)
        lap = n + s + e + w - 4.0 * u
        out.append(u + factor * (diffusion[c] * lap - adv))
    return out


def cycle(n_t, n_g, h, init_ref, ge_ref, vel_ref, cor_ref, rel_ref,
          ini, ge, vel, bufs, side, work, held, send_sem, recv_sem):
    t, g = lax.axis_index("tm"), lax.axis_index("gy")
    pos, cluster = lax.rem(t, GROUP), lax.div(t, GROUP)
    F = FINE
    level_one, coarsest = FINE * time_step, FINE * GROUP * time_step
    up, down = g < n_g - 1, g > 0
    last = GROUP - 1
    tiles = ge_ref.shape[-1] // LANES
    bbuf, lbuf, dbuf = bufs.at[0], bufs.at[1], bufs.at[2]
    abuf, sbuf = side.at[0], side.at[1]
    source, forcing, state, corr = held.at[0], held.at[1], held.at[2], held.at[3]

    def conj(*conditions):
        total = conditions[0]
        for other in conditions[1:]:
            total = jnp.logical_and(total, other)
        return total

    sends = []

    barrier = pltpu.get_barrier_semaphore()
    count = jnp.int32(0)
    for dt in (-GROUP, -1, 0, 1, GROUP):
        for dg in (-1, 0, 1):
            if dt == 0 and dg == 0:
                continue
            ok = conj(t + dt >= 0, t + dt < n_t, g + dg >= 0, g + dg < n_g)
            if abs(dt) == GROUP:
                ok = conj(ok, pos == last)
            @pl.when(ok)
            def _():
                pl.semaphore_signal(barrier, inc=1, device_id={"tm": t + dt, "gy": g + dg},
                                    device_id_type=pl.DeviceIdType.MESH)
            count = count + ok.astype(jnp.int32)

    def spread(src, index, dst, at):
        for c in range(src.shape[-3]):
            for k in range(tiles):
                rows = (src[index, c, :, k * LANES : (k + 1) * LANES] if index is not None
                        else src[c, :, k * LANES : (k + 1) * LANES])
                dst[at : at + h, c, k, :] = rows

    spread(vel_ref, 0, vel, F)
    spread(ge_ref, 0, ge, 0)
    @pl.when(jnp.logical_or(t == 0, t == last))
    def _():
        spread(init_ref, None, ini, 0)

    @pl.when(g == 0)
    def _():
        for b in (bbuf, lbuf, dbuf):
            b[0:F] = jnp.zeros((F,) + b.shape[1:], jnp.float32)
        for b in (abuf, sbuf):
            b[0:1] = jnp.zeros((1,) + b.shape[1:], jnp.float32)
        vel[0:F] = jnp.zeros((F,) + vel.shape[1:], jnp.float32)
    @pl.when(g == n_g - 1)
    def _():
        for b in (bbuf, lbuf, dbuf):
            b[F + h :] = jnp.zeros((F,) + b.shape[1:], jnp.float32)
        for b in (abuf, sbuf):
            b[1 + h :] = jnp.zeros((1,) + b.shape[1:], jnp.float32)
        vel[F + h :] = jnp.zeros((F,) + vel.shape[1:], jnp.float32)

    pl.semaphore_wait(barrier, count)

    def copy(src, dst, kind, dt, dg):
        return pltpu.make_async_remote_copy(
            src_ref=src, dst_ref=dst, send_sem=send_sem.at[len(sends)], recv_sem=recv_sem.at[kind],
            device_id={"tm": t + dt, "gy": g + dg}, device_id_type=pl.DeviceIdType.MESH)

    def edges(src, dst, kinds, dt, width, condition):
        for ok, rows, at, kind, dg in (
            (up, src.at[h - width : h], dst.at[0:width], kinds[0], 1),
            (down, src.at[0:width], dst.at[width + h : 2 * width + h], kinds[1], -1),
        ):
            move = copy(rows, at, kind, dt, dg)
            allowed = ok if condition is None else conj(ok, condition)
            pl.when(allowed)(move.start)
            sends.append((allowed, move))

    def whole(src, dst, kind, dt, width, condition):
        move = copy(src, dst.at[width : width + h], kind, dt, 0)
        pl.when(condition)(move.start)
        sends.append((condition, move))

    def arrived(dst, kinds, width, center=True, condition=None):
        def wait():
            if center:
                copy(held.at[0], dst.at[width : width + h], kinds[0], 0, 0).wait_recv()
            @pl.when(down)
            def _():
                copy(dst.at[0:width], dst.at[0:width], kinds[1], 0, 0).wait_recv()
            @pl.when(up)
            def _():
                copy(dst.at[0:width], dst.at[width + h : 2 * width + h], kinds[2], 0, 0).wait_recv()
        if condition is None:
            wait()
        else:
            pl.when(condition)(wait)

    center = vel.at[F : F + h]
    follows = t + 1 < n_t
    leaps = conj(pos == last, t + GROUP < n_t)
    edges(ge, bbuf, (BLO, BHI), 1, F, follows)
    whole(ge, bbuf, BC, 1, F, follows)
    edges(center, vel, (VLO, VHI), 0, F, None)
    edges(ini, bbuf, (BLO, BHI), 0, F, t == 0)
    edges(ini, abuf, (ALO, AHI), 0, 1, t == last)
    edges(ge, abuf, (ALO, AHI), GROUP, 1, leaps)
    whole(ge, abuf, AC, GROUP, 1, leaps)

    @pl.when(t == 0)
    def _():
        bbuf[F : F + h] = ini[...]
    @pl.when(t == last)
    def _():
        abuf[1 : 1 + h] = ini[...]

    def blocks(first, total):
        done = 0
        while done < total:
            size = min(BLOCK, total - done)
            yield first + done, size
            done += size

    def fine(src, final):
        here = src
        for section in range(F):
            halo = F - section - 1
            target = work.at[section % 2]
            for row, size in blocks(-halo, h + 2 * halo):
                new = step_rows(here, F + row, vel, F + row, size, time_step)
                if section == F - 1:
                    final(row, size, new)
                    continue
                for c in range(3):
                    value = new[c]
                    for i in range(size):
                        if row + i < 0:
                            target[F + row + i, c] = jnp.where(down, value[i], 0.0)
                        elif row + i >= h:
                            target[F + row + i, c] = jnp.where(up, value[i], 0.0)
                        else:
                            target[F + row + i, c] = value[i]
            here = target

    arrived(vel, (None, VLO, VHI), F, center=False)
    pl.when(t > 0)(lambda: copy(held.at[0], bbuf.at[F : F + h], BC, 0, 0).wait_recv())
    arrived(bbuf, (None, BLO, BHI), F, center=False)

    def keep_source(row, size, new):
        coarse = step_rows(bbuf, F + row, vel, F + row, size, level_one)
        for c in range(3):
            value = new[c] - coarse[c]
            source[row : row + size, c] = value
            state[row : row + size, c] = coarse[c] + value

    fine(bbuf, keep_source)

    def forward(src, dst, width, factor, added, target):
        for row, size in blocks(0, h):
            new = step_rows(src, width + row, vel, F + row, size, factor)
            for c in range(3):
                target[row : row + size, c] = new[c] + added[row : row + size, c]

    @pl.when(pos > 0)
    def _():
        arrived(lbuf, (LC, LLO, LHI), F)
        forward(lbuf, None, F, level_one, source, state)

    edges(state, lbuf, (LLO, LHI), 1, F, pos < last)
    whole(state, lbuf, LC, 1, F, pos < last)

    @pl.when(pos == last)
    def _():
        @pl.when(cluster > 0)
        def _():
            copy(held.at[0], abuf.at[1 : 1 + h], AC, 0, 0).wait_recv()
        arrived(abuf, (None, ALO, AHI), 1, center=False)
        for row, size in blocks(0, h):
            new = step_rows(abuf, 1 + row, vel, F + row, size, coarsest)
            for c in range(3):
                value = state[row : row + size, c] - new[c]
                forcing[row : row + size, c] = value
                corr[row : row + size, c] = new[c] + value
        @pl.when(cluster > 0)
        def _():
            arrived(sbuf, (SC, SLO, SHI), 1)
            forward(sbuf, None, 1, coarsest, forcing, corr)

    @pl.when(conj(pos < last, cluster == 0))
    def _():
        corr[...] = state[...]

    @pl.when(conj(pos < last, cluster > 0))
    def _():
        arrived(dbuf, (DC, DLO, DHI), F)
        forward(dbuf, None, F, level_one, source, corr)

    onward = conj(follows, jnp.logical_or(cluster > 0, pos == last))
    edges(corr, dbuf, (DLO, DHI), 1, F, onward)
    whole(corr, dbuf, DC, 1, F, onward)
    edges(corr, sbuf, (SLO, SHI), GROUP, 1, leaps)
    whole(corr, sbuf, SC, GROUP, 1, leaps)

    for c in range(3):
        for k in range(tiles):
            cor_ref[0, c, :, k * LANES : (k + 1) * LANES] = corr[:, c, k, :]

    arrived(dbuf, (DC, DLO, DHI), F, condition=conj(pos == last, cluster > 0))

    chosen = jnp.where(cluster > 0, 2, jnp.where(t > 0, 1, 0))

    def keep_relaxed(row, size, new):
        for c in range(3):
            source[row : row + size, c] = new[c]

    fine(bufs.at[chosen], keep_relaxed)
    for c in range(3):
        for k in range(tiles):
            rel_ref[0, c, :, k * LANES : (k + 1) * LANES] = source[:, c, k, :]

    for allowed, move in sends:
        pl.when(allowed)(move.wait_send)


def solution(mesh):
    n_t, n_g = mesh.shape["tm"], mesh.shape["gy"]

    def per_device(initial_state, guessed_ends, velocity):
        _, h, nx = initial_state.shape
        sub = nx // LANES
        F = FINE
        out = jax.ShapeDtypeStruct(guessed_ends.shape, jnp.float32)
        f32 = lambda *shape: pltpu.VMEM(shape + (sub, LANES), jnp.float32)
        whole = pl.BlockSpec(memory_space=pltpu.VMEM)
        return pl.pallas_call(
            functools.partial(cycle, n_t, n_g, h),
            out_shape=(out, out),
            in_specs=[whole] * 3,
            out_specs=(whole, whole),
            scratch_shapes=[
                f32(h, 3), f32(h, 3), f32(h + 2 * F, 2), f32(3, h + 2 * F, 3), f32(2, h + 2, 3),
                f32(2, h + 2 * F, 3), f32(4, h, 3),
                pltpu.SemaphoreType.DMA((SENDS,)), pltpu.SemaphoreType.DMA((KINDS,)),
            ],
            compiler_params=pltpu.CompilerParams(collective_id=0, has_side_effects=True),
            name="cycle",
        )(initial_state, guessed_ends, velocity)

    across = P("tm", None, "gy", None)
    return jax.shard_map(
        per_device, mesh=mesh, in_specs=(P(None, "gy", None), across, across),
        out_specs=(across, across), check_vma=False)
```

```python
import functools

import jax
import jax.numpy as jnp
from jax import lax
from jax.experimental import pallas as pl
from jax.experimental.pallas import tpu as pltpu
from jax.sharding import PartitionSpec as P

FINE = 4
GROUP = 4
LANES = 128
BLOCK = 4

diffusion = (0.05, 0.15, 0.4)
kappa_coupling = 0.1
time_step = 0.0125

VLO, VHI, BC, BLO, BHI, AC, ALO, AHI, LC, LLO, LHI, DC, DLO, DHI, SC, SLO, SHI, KINDS = range(18)
SENDS = 40


def shifted(x, by):
    sub, lanes = x.shape[-2:]
    lane = lax.broadcasted_iota(jnp.int32, (1, sub, lanes), 2)
    if by == 1:
        turned = pltpu.roll(x, lanes - 1, 2)
        return jnp.where(lane == lanes - 1, pltpu.roll(turned, sub - 1, 1), turned)
    turned = pltpu.roll(x, 1, 2)
    return jnp.where(lane == 0, pltpu.roll(turned, 1, 1), turned)


def step_rows(src, first, vel, vfirst, count, factor):
    vx, vy = vel[vfirst : vfirst + count, 0], vel[vfirst : vfirst + count, 1]
    u0 = src[first : first + count, 0]
    u1 = src[first : first + count, 1]
    ax = vx + kappa_coupling * u0
    ay = vy + kappa_coupling * u1
    axp, axn = jnp.maximum(ax, 0.0), jnp.minimum(ax, 0.0)
    ayp, ayn = jnp.maximum(ay, 0.0), jnp.minimum(ay, 0.0)
    out = []
    for c in range(3):
        u = (u0, u1)[c] if c < 2 else src[first : first + count, 2]
        n = src[first + 1 : first + 1 + count, c]
        s = src[first - 1 : first - 1 + count, c]
        e, w = shifted(u, 1), shifted(u, -1)
        adv = axp * (u - w) + axn * (e - u)
        adv = adv + ayp * (u - s) + ayn * (n - u)
        lap = n + s + e + w - 4.0 * u
        out.append(u + factor * (diffusion[c] * lap - adv))
    return out


def cycle(n_t, n_g, h, init_ref, ge_ref, vel_ref, begin_ref, cor_ref, vel,
          ini, ge, bbuf, bufs, side, work, held, send_sem, recv_sem):
    t, g = lax.axis_index("tm"), lax.axis_index("gy")
    pos, cluster = lax.rem(t, GROUP), lax.div(t, GROUP)
    F = FINE
    level_one, coarsest = FINE * time_step, FINE * GROUP * time_step
    up, down = g < n_g - 1, g > 0
    last = GROUP - 1
    tiles = ge_ref.shape[-1] // LANES
    lbuf, dbuf = bufs.at[0], bufs.at[1]
    abuf, sbuf = side.at[0], side.at[1]
    source, forcing, state, corr = held.at[0], held.at[1], held.at[2], held.at[3]
    even = lax.rem(pos, 2) == 0
    H = F + 1

    def conj(*conditions):
        total = conditions[0]
        for other in conditions[1:]:
            total = jnp.logical_and(total, other)
        return total

    sends = []

    @pl.when(g == 0)
    def _():
        bbuf[0:H] = jnp.zeros((H,) + bbuf.shape[1:], jnp.float32)
        for b in (lbuf, dbuf):
            b[0:F] = jnp.zeros((F,) + b.shape[1:], jnp.float32)
        for b in (abuf, sbuf):
            b[0:1] = jnp.zeros((1,) + b.shape[1:], jnp.float32)
        vel[0:F] = jnp.zeros((F,) + vel.shape[1:], jnp.float32)
    @pl.when(g == n_g - 1)
    def _():
        bbuf[H + h :] = jnp.zeros((H,) + bbuf.shape[1:], jnp.float32)
        for b in (lbuf, dbuf):
            b[F + h :] = jnp.zeros((F,) + b.shape[1:], jnp.float32)
        for b in (abuf, sbuf):
            b[1 + h :] = jnp.zeros((1,) + b.shape[1:], jnp.float32)
        vel[F + h :] = jnp.zeros((F,) + vel.shape[1:], jnp.float32)

    barrier = pltpu.get_barrier_semaphore()
    count = jnp.int32(0)
    for dt in (-GROUP, -1, 0, 1, GROUP):
        for dg in (-1, 0, 1):
            if dt == 0 and dg == 0:
                continue
            ok = conj(t + dt >= 0, t + dt < n_t, g + dg >= 0, g + dg < n_g)
            if abs(dt) == GROUP:
                ok = conj(ok, pos == last)
            @pl.when(ok)
            def _():
                pl.semaphore_signal(barrier, inc=1, device_id={"tm": t + dt, "gy": g + dg},
                                    device_id_type=pl.DeviceIdType.MESH)
            count = count + ok.astype(jnp.int32)

    def spread(src, index, dst, at):
        for c in range(src.shape[-3]):
            for k in range(tiles):
                rows = (src[index, c, :, k * LANES : (k + 1) * LANES] if index is not None
                        else src[c, :, k * LANES : (k + 1) * LANES])
                dst[at : at + h, c, k, :] = rows

    spread(vel_ref, 0, vel, F)
    spread(ge_ref, 0, ge, 0)
    @pl.when(jnp.logical_or(t == 0, t == last))
    def _():
        spread(init_ref, None, ini, 0)

    pl.semaphore_wait(barrier, count)

    def copy(src, dst, kind, dt, dg):
        return pltpu.make_async_remote_copy(
            src_ref=src, dst_ref=dst, send_sem=send_sem.at[len(sends)], recv_sem=recv_sem.at[kind],
            device_id={"tm": t + dt, "gy": g + dg}, device_id_type=pl.DeviceIdType.MESH)

    def edges(src, dst, kinds, dt, width, condition):
        for ok, rows, at, kind, dg in (
            (up, src.at[h - width : h], dst.at[0:width], kinds[0], 1),
            (down, src.at[0:width], dst.at[width + h : 2 * width + h], kinds[1], -1),
        ):
            move = copy(rows, at, kind, dt, dg)
            allowed = ok if condition is None else conj(ok, condition)
            pl.when(allowed)(move.start)
            sends.append((allowed, move))

    def whole(src, dst, kind, dt, width, condition):
        move = copy(src, dst.at[width : width + h], kind, dt, 0)
        pl.when(condition)(move.start)
        sends.append((condition, move))

    def arrived(dst, kinds, width, center=True, condition=None):
        def wait():
            if center:
                copy(held.at[0, 1 : 1 + h], dst.at[width : width + h], kinds[0], 0, 0).wait_recv()
            @pl.when(down)
            def _():
                copy(dst.at[0:width], dst.at[0:width], kinds[1], 0, 0).wait_recv()
            @pl.when(up)
            def _():
                copy(dst.at[0:width], dst.at[width + h : 2 * width + h], kinds[2], 0, 0).wait_recv()
        if condition is None:
            wait()
        else:
            pl.when(condition)(wait)

    center = vel.at[F : F + h]
    follows = t + 1 < n_t
    leaps = conj(pos == last, t + GROUP < n_t)
    edges(ge, bbuf, (BLO, BHI), 1, H, follows)
    whole(ge, bbuf, BC, 1, H, follows)
    edges(center, vel, (VLO, VHI), 0, F, None)
    edges(ini, bbuf, (BLO, BHI), 0, H, t == 0)
    edges(ini, abuf, (ALO, AHI), 0, 1, t == last)
    edges(ge, abuf, (ALO, AHI), GROUP, 1, leaps)
    whole(ge, abuf, AC, GROUP, 1, leaps)

    @pl.when(t == 0)
    def _():
        bbuf[H : H + h] = ini[...]
    @pl.when(t == last)
    def _():
        abuf[1 : 1 + h] = ini[...]

    def blocks(first, total):
        done = 0
        while done < total:
            size = min(BLOCK, total - done)
            yield first + done, size
            done += size

    def put(target, at, row, size, new):
        for c in range(3):
            for i in range(size):
                value = new[c][i]
                if row + i < 0:
                    value = jnp.where(down, value, 0.0)
                elif row + i >= h:
                    value = jnp.where(up, value, 0.0)
                target[at + row + i, c] = value

    arrived(vel, (None, VLO, VHI), F, center=False)
    pl.when(t > 0)(lambda: copy(held.at[0, 1 : 1 + h], bbuf.at[H : H + h], BC, 0, 0).wait_recv())
    arrived(bbuf, (None, BLO, BHI), H, center=False)

    here = bbuf
    for section in range(F):
        halo = F - section
        for row, size in blocks(-halo, h + 2 * halo):
            new = step_rows(here, H + row, vel, F + row, size, time_step)
            if section < F - 1:
                put(work.at[section % 2], H, row, size, new)
                continue
            coarse = step_rows(bbuf, H + row, vel, F + row, size, level_one)
            value = [new[c] - coarse[c] for c in range(3)]
            put(source, 1, row, size, value)
            put(state, 1, row, size, [coarse[c] + value[c] for c in range(3)])
        here = work.at[section % 2]

    def forward(src, width, factor, added, target, extra):
        for row, size in blocks(-extra, h + 2 * extra):
            new = step_rows(src, width + row, vel, F + row, size, factor)
            put(target, 1, row, size,
                [new[c] + added[1 + row : 1 + row + size, c] for c in range(3)])

    def onto_next(src, dst, kinds, condition):
        center, lo, hi = kinds
        wide = conj(condition, even)
        move = copy(src, dst.at[F - 1 : F + 1 + h], center, 1, 0)
        pl.when(wide)(move.start)
        sends.append((wide, move))
        for ok, at, to, kind, dg in (
            (up, 1 + h - F, 0, lo, 1), (down, 2, F + h + 1, hi, -1),
        ):
            allowed = conj(wide, ok)
            move = copy(src.at[at : at + F - 1], dst.at[to : to + F - 1], kind, 1, dg)
            pl.when(allowed)(move.start)
            sends.append((allowed, move))
        narrow = conj(condition, jnp.logical_not(even))
        edges(src.at[1 : 1 + h], dst, (lo, hi), 1, F, narrow)
        whole(src.at[1 : 1 + h], dst, center, 1, F, narrow)

    def from_previous(dst, kinds, target):
        @pl.when(even)
        def _():
            arrived(dst, kinds, F)
            forward(dst, F, level_one, source, target, 1)
        @pl.when(jnp.logical_not(even))
        def _():
            copy(held.at[0], dst.at[F - 1 : F + 1 + h], kinds[0], 0, 0).wait_recv()
            forward(dst, F, level_one, source, target, 0)

    def outer_rows(dst, kinds, condition):
        @pl.when(conj(condition, down))
        def _():
            copy(held.at[0, 0 : F - 1], dst.at[0 : F - 1], kinds[1], 0, 0).wait_recv()
        @pl.when(conj(condition, up))
        def _():
            copy(held.at[0, 0 : F - 1], dst.at[F + h + 1 : 2 * F + h], kinds[2], 0, 0).wait_recv()

    odd = jnp.logical_not(even)
    L, D, S = (LC, LLO, LHI), (DC, DLO, DHI), (SC, SLO, SHI)
    pl.when(pos > 0)(lambda: from_previous(lbuf, L, state))
    onto_next(state, lbuf, L, pos < last)

    @pl.when(pos == last)
    def _():
        @pl.when(cluster > 0)
        def _():
            copy(held.at[0, 1 : 1 + h], abuf.at[1 : 1 + h], AC, 0, 0).wait_recv()
        arrived(abuf, (None, ALO, AHI), 1, center=False)
        for row, size in blocks(0, h):
            new = step_rows(abuf, 1 + row, vel, F + row, size, coarsest)
            value = [state[1 + row : 1 + row + size, c] - new[c] for c in range(3)]
            put(forcing, 1, row, size, value)
            put(corr, 1, row, size, [new[c] + value[c] for c in range(3)])
        @pl.when(cluster > 0)
        def _():
            arrived(sbuf, S, 1)
            forward(sbuf, 1, coarsest, forcing, corr, 0)

    @pl.when(conj(pos < last, cluster == 0))
    def _():
        corr[...] = state[...]

    pl.when(conj(pos < last, cluster > 0))(lambda: from_previous(dbuf, D, corr))

    onward = conj(follows, jnp.logical_or(cluster > 0, pos == last))
    onto_next(corr, dbuf, D, onward)
    edges(corr.at[1 : 1 + h], sbuf, (SLO, SHI), GROUP, 1, leaps)
    whole(corr.at[1 : 1 + h], sbuf, SC, GROUP, 1, leaps)
    cor_ref[...] = corr[1 : 1 + h]

    @pl.when(conj(pos == last, cluster > 0))
    def _():
        copy(held.at[0], dbuf.at[F - 1 : F + 1 + h], DC, 0, 0).wait_recv()
    outer_rows(lbuf, L, odd)
    outer_rows(dbuf, D, conj(odd, cluster > 0))

    @pl.when(t == 0)
    def _():
        begin_ref[...] = bbuf[1 : 1 + h + 2 * F]
    @pl.when(t > 0)
    def _():
        begin_ref[...] = bufs[jnp.where(cluster > 0, 1, 0)]

    for allowed, move in sends:
        pl.when(allowed)(move.wait_send)


def relax(n_g, h, begin, cor, vel, cor_ref, rel_ref, work):
    g = lax.axis_index("gy")
    up, down = g < n_g - 1, g > 0
    F = FINE
    tiles = cor_ref.shape[-1] // LANES
    for c in range(3):
        for k in range(tiles):
            cor_ref[0, c, :, k * LANES : (k + 1) * LANES] = cor[:, c, k, :]
    here = begin
    for section in range(F):
        halo = F - section - 1
        target = work.at[section % 2]
        row = -halo
        while row < h + halo:
            size = min(BLOCK, h + halo - row)
            new = step_rows(here, F + row, vel, F + row, size, time_step)
            for c in range(3):
                for i in range(size):
                    value = new[c][i]
                    if row + i < 0:
                        value = jnp.where(down, value, 0.0)
                    elif row + i >= h:
                        value = jnp.where(up, value, 0.0)
                    target[F + row + i, c] = value
            row += size
        here = target
    for c in range(3):
        for k in range(tiles):
            rel_ref[0, c, :, k * LANES : (k + 1) * LANES] = here[F : F + h, c, k, :]


def solution(mesh):
    n_t, n_g = mesh.shape["tm"], mesh.shape["gy"]

    def per_device(initial_state, guessed_ends, velocity):
        _, h, nx = initial_state.shape
        sub = nx // LANES
        F = FINE
        out = jax.ShapeDtypeStruct(guessed_ends.shape, jnp.float32)
        f32 = lambda *shape: pltpu.VMEM(shape + (sub, LANES), jnp.float32)
        whole = pl.BlockSpec(memory_space=pltpu.VMEM)
        shape = lambda *dims: jax.ShapeDtypeStruct(dims + (sub, LANES), jnp.float32)
        begin, corrected, flow = pl.pallas_call(
            functools.partial(cycle, n_t, n_g, h),
            out_shape=(shape(h + 2 * F, 3), shape(h, 3), shape(h + 2 * F, 2)),
            in_specs=[whole] * 3,
            out_specs=(whole,) * 3,
            scratch_shapes=[
                f32(h, 3), f32(h, 3), f32(h + 2 * F + 2, 3), f32(2, h + 2 * F, 3),
                f32(2, h + 2, 3), f32(2, h + 2 * F + 2, 3), f32(4, h + 2, 3),
                pltpu.SemaphoreType.DMA((SENDS,)), pltpu.SemaphoreType.DMA((KINDS,)),
            ],
            compiler_params=pltpu.CompilerParams(
                collective_id=0, has_side_effects=True, vmem_limit_bytes=16 * 2**20),
            name="cycle",
        )(initial_state, guessed_ends, velocity)
        return pl.pallas_call(
            functools.partial(relax, n_g, h),
            out_shape=(out, out),
            in_specs=[whole] * 3,
            out_specs=(whole, whole),
            scratch_shapes=[f32(2, h + 2 * F, 3)],
            compiler_params=pltpu.CompilerParams(vmem_limit_bytes=16 * 2**20),
            name="relax",
        )(begin, corrected, flow)

    across = P("tm", None, "gy", None)
    return jax.shard_map(
        per_device, mesh=mesh, in_specs=(P(None, "gy", None), across, across),
        out_specs=(across, across), check_vma=False)
```

```python
import functools

import jax
import jax.numpy as jnp
from jax import lax
from jax.experimental import pallas as pl
from jax.experimental.pallas import tpu as pltpu
from jax.sharding import PartitionSpec as P

FINE = 4
GROUP = 4
LANES = 128
BLOCK = 4

diffusion = (0.05, 0.15, 0.4)
kappa_coupling = 0.1
time_step = 0.0125

VLO, VHI, BC, BLO, BHI, AC, ALO, AHI, LC, LLO, LHI, DC, DLO, DHI, SC, SLO, SHI, LOL, LOH, DOL, DOH, KINDS = range(22)
SENDS = 40


def shifted(x, by):
    sub, lanes = x.shape[-2:]
    lane = lax.broadcasted_iota(jnp.int32, (1, sub, lanes), 2)
    if by == 1:
        turned = pltpu.roll(x, lanes - 1, 2)
        return jnp.where(lane == lanes - 1, pltpu.roll(turned, sub - 1, 1), turned)
    turned = pltpu.roll(x, 1, 2)
    return jnp.where(lane == 0, pltpu.roll(turned, 1, 1), turned)


def step_rows(src, first, vel, vfirst, count, factor):
    vx, vy = vel[vfirst : vfirst + count, 0], vel[vfirst : vfirst + count, 1]
    u0 = src[first : first + count, 0]
    u1 = src[first : first + count, 1]
    ax = vx + kappa_coupling * u0
    ay = vy + kappa_coupling * u1
    axp, axn = jnp.maximum(ax, 0.0), jnp.minimum(ax, 0.0)
    ayp, ayn = jnp.maximum(ay, 0.0), jnp.minimum(ay, 0.0)
    out = []
    for c in range(3):
        u = (u0, u1)[c] if c < 2 else src[first : first + count, 2]
        n = src[first + 1 : first + 1 + count, c]
        s = src[first - 1 : first - 1 + count, c]
        e, w = shifted(u, 1), shifted(u, -1)
        adv = axp * (u - w) + axn * (e - u)
        adv = adv + ayp * (u - s) + ayn * (n - u)
        lap = n + s + e + w - 4.0 * u
        out.append(u + factor * (diffusion[c] * lap - adv))
    return out


def cycle(n_t, n_g, h, init_ref, ge_ref, vel_ref, begin_ref, cor_ref, vel,
          ini, ge, bbuf, bufs, side, work, held, send_sem, recv_sem):
    t, g = lax.axis_index("tm"), lax.axis_index("gy")
    pos, cluster = lax.rem(t, GROUP), lax.div(t, GROUP)
    F = FINE
    level_one, coarsest = FINE * time_step, FINE * GROUP * time_step
    up, down = g < n_g - 1, g > 0
    last = GROUP - 1
    tiles = ge_ref.shape[-1] // LANES
    lbuf, dbuf = bufs.at[0], bufs.at[1]
    abuf, sbuf = side.at[0], side.at[1]
    source, forcing, state, corr = held.at[0], held.at[1], held.at[2], held.at[3]
    even = lax.rem(pos, 2) == 0
    H = F + 1

    def conj(*conditions):
        total = conditions[0]
        for other in conditions[1:]:
            total = jnp.logical_and(total, other)
        return total

    sends = []

    @pl.when(g == 0)
    def _():
        bbuf[0:H] = jnp.zeros((H,) + bbuf.shape[1:], jnp.float32)
        for b in (lbuf, dbuf):
            b[0:F] = jnp.zeros((F,) + b.shape[1:], jnp.float32)
        for b in (abuf, sbuf):
            b[0:1] = jnp.zeros((1,) + b.shape[1:], jnp.float32)
        vel[0:F] = jnp.zeros((F,) + vel.shape[1:], jnp.float32)
    @pl.when(g == n_g - 1)
    def _():
        bbuf[H + h :] = jnp.zeros((H,) + bbuf.shape[1:], jnp.float32)
        for b in (lbuf, dbuf):
            b[F + h :] = jnp.zeros((F,) + b.shape[1:], jnp.float32)
        for b in (abuf, sbuf):
            b[1 + h :] = jnp.zeros((1,) + b.shape[1:], jnp.float32)
        vel[F + h :] = jnp.zeros((F,) + vel.shape[1:], jnp.float32)

    barrier = pltpu.get_barrier_semaphore()
    count = jnp.int32(0)
    for dt in (-GROUP, -1, 0, 1, GROUP):
        for dg in (-1, 0, 1):
            if dt == 0 and dg == 0:
                continue
            ok = conj(t + dt >= 0, t + dt < n_t, g + dg >= 0, g + dg < n_g)
            if abs(dt) == GROUP:
                ok = conj(ok, pos == last)
            @pl.when(ok)
            def _():
                pl.semaphore_signal(barrier, inc=1, device_id={"tm": t + dt, "gy": g + dg},
                                    device_id_type=pl.DeviceIdType.MESH)
            count = count + ok.astype(jnp.int32)

    def spread(src, index, dst, at):
        for c in range(src.shape[-3]):
            for k in range(tiles):
                rows = (src[index, c, :, k * LANES : (k + 1) * LANES] if index is not None
                        else src[c, :, k * LANES : (k + 1) * LANES])
                dst[at : at + h, c, k, :] = rows

    spread(vel_ref, 0, vel, F)
    spread(ge_ref, 0, ge, 0)
    @pl.when(jnp.logical_or(t == 0, t == last))
    def _():
        spread(init_ref, None, ini, 0)

    pl.semaphore_wait(barrier, count)

    def copy(src, dst, kind, dt, dg):
        return pltpu.make_async_remote_copy(
            src_ref=src, dst_ref=dst, send_sem=send_sem.at[len(sends)], recv_sem=recv_sem.at[kind],
            device_id={"tm": t + dt, "gy": g + dg}, device_id_type=pl.DeviceIdType.MESH)

    def edges(src, dst, kinds, dt, width, condition):
        for ok, rows, at, kind, dg in (
            (up, src.at[h - width : h], dst.at[0:width], kinds[0], 1),
            (down, src.at[0:width], dst.at[width + h : 2 * width + h], kinds[1], -1),
        ):
            move = copy(rows, at, kind, dt, dg)
            allowed = ok if condition is None else conj(ok, condition)
            pl.when(allowed)(move.start)
            sends.append((allowed, move))

    def whole(src, dst, kind, dt, width, condition):
        move = copy(src, dst.at[width : width + h], kind, dt, 0)
        pl.when(condition)(move.start)
        sends.append((condition, move))

    def arrived(dst, kinds, width, center=True, condition=None):
        def wait():
            if center:
                copy(held.at[0, 1 : 1 + h], dst.at[width : width + h], kinds[0], 0, 0).wait_recv()
            @pl.when(down)
            def _():
                copy(dst.at[0:width], dst.at[0:width], kinds[1], 0, 0).wait_recv()
            @pl.when(up)
            def _():
                copy(dst.at[0:width], dst.at[width + h : 2 * width + h], kinds[2], 0, 0).wait_recv()
        if condition is None:
            wait()
        else:
            pl.when(condition)(wait)

    center = vel.at[F : F + h]
    follows = t + 1 < n_t
    leaps = conj(pos == last, t + GROUP < n_t)
    edges(ge, bbuf, (BLO, BHI), 1, H, follows)
    whole(ge, bbuf, BC, 1, H, follows)
    edges(center, vel, (VLO, VHI), 0, F, None)
    edges(ini, bbuf, (BLO, BHI), 0, H, t == 0)
    edges(ini, abuf, (ALO, AHI), 0, 1, t == last)
    edges(ge, abuf, (ALO, AHI), GROUP, 1, leaps)
    whole(ge, abuf, AC, GROUP, 1, leaps)

    @pl.when(t == 0)
    def _():
        bbuf[H : H + h] = ini[...]
    @pl.when(t == last)
    def _():
        abuf[1 : 1 + h] = ini[...]

    def blocks(first, total):
        done = 0
        while done < total:
            size = min(BLOCK, total - done)
            yield first + done, size
            done += size

    def put(target, at, row, size, new):
        for c in range(3):
            for i in range(size):
                value = new[c][i]
                if row + i < 0:
                    value = jnp.where(down, value, 0.0)
                elif row + i >= h:
                    value = jnp.where(up, value, 0.0)
                target[at + row + i, c] = value

    arrived(vel, (None, VLO, VHI), F, center=False)
    pl.when(t > 0)(lambda: copy(held.at[0, 1 : 1 + h], bbuf.at[H : H + h], BC, 0, 0).wait_recv())
    arrived(bbuf, (None, BLO, BHI), H, center=False)

    here = bbuf
    for section in range(F):
        halo = F - section
        for row, size in blocks(-halo, h + 2 * halo):
            new = step_rows(here, H + row, vel, F + row, size, time_step)
            if section < F - 1:
                put(work.at[section % 2], H, row, size, new)
                continue
            coarse = step_rows(bbuf, H + row, vel, F + row, size, level_one)
            value = [new[c] - coarse[c] for c in range(3)]
            put(source, 1, row, size, value)
            put(state, 1, row, size, [coarse[c] + value[c] for c in range(3)])
        here = work.at[section % 2]

    def forward(src, width, factor, added, target, extra):
        for row, size in blocks(-extra, h + 2 * extra):
            new = step_rows(src, width + row, vel, F + row, size, factor)
            put(target, 1, row, size,
                [new[c] + added[1 + row : 1 + row + size, c] for c in range(3)])

    def onto_next(src, dst, kinds, condition):
        center, lo, hi, outer_lo, outer_hi = kinds
        wide = conj(condition, even)
        move = copy(src, dst.at[F - 1 : F + 1 + h], center, 1, 0)
        pl.when(wide)(move.start)
        sends.append((wide, move))
        for ok, at, to, kind, dg in (
            (up, 1 + h - F, 0, lo, 1), (down, 2, F + h + 1, hi, -1),
        ):
            allowed = conj(wide, ok)
            move = copy(src.at[at : at + F - 1], dst.at[to : to + F - 1], kind, 1, dg)
            pl.when(allowed)(move.start)
            sends.append((allowed, move))
        narrow = conj(condition, jnp.logical_not(even))
        edges(src.at[1 : 1 + h], dst.at[F - 2 : F + h + 2], (lo, hi), 1, 2, narrow)
        whole(src.at[1 : 1 + h], dst, center, 1, F, narrow)
        for ok, at, to, kind, dg in (
            (up, 1 + h - F, 0, outer_lo, 1), (down, 3, F + h + 2, outer_hi, -1),
        ):
            allowed = conj(narrow, ok)
            move = copy(src.at[at : at + F - 2], dst.at[to : to + F - 2], kind, 1, dg)
            pl.when(allowed)(move.start)
            sends.append((allowed, move))

    def from_previous(dst, kinds, target):
        @pl.when(even)
        def _():
            copy(held.at[0, 1 : 1 + h], dst.at[F : F + h], kinds[0], 0, 0).wait_recv()
            arrived(dst.at[F - 2 : F + h + 2], kinds, 2, center=False)
            forward(dst, F, level_one, source, target, 1)
        @pl.when(jnp.logical_not(even))
        def _():
            copy(held.at[0], dst.at[F - 1 : F + 1 + h], kinds[0], 0, 0).wait_recv()
            forward(dst, F, level_one, source, target, 0)

    def outer_rows(dst, lo, hi, width, condition):
        @pl.when(conj(condition, down))
        def _():
            copy(held.at[0, 0:width], dst.at[0:width], lo, 0, 0).wait_recv()
        @pl.when(conj(condition, up))
        def _():
            copy(held.at[0, 0:width], dst.at[2 * F + h - width :], hi, 0, 0).wait_recv()

    odd = jnp.logical_not(even)
    L, D, S = (LC, LLO, LHI, LOL, LOH), (DC, DLO, DHI, DOL, DOH), (SC, SLO, SHI)
    @pl.when(pos == last)
    def _():
        @pl.when(cluster > 0)
        def _():
            copy(held.at[0, 1 : 1 + h], abuf.at[1 : 1 + h], AC, 0, 0).wait_recv()
        arrived(abuf, (None, ALO, AHI), 1, center=False)
        for row, size in blocks(0, h):
            put(corr, 1, row, size, step_rows(abuf, 1 + row, vel, F + row, size, coarsest))

    pl.when(pos > 0)(lambda: from_previous(lbuf, L, state))
    onto_next(state, lbuf, L, pos < last)

    @pl.when(pos == last)
    def _():
        for row, size in blocks(1, h):
            for c in range(3):
                begun = corr[row : row + size, c]
                value = state[row : row + size, c] - begun
                forcing[row : row + size, c] = value
                corr[row : row + size, c] = begun + value
        @pl.when(cluster > 0)
        def _():
            arrived(sbuf, S, 1)
            forward(sbuf, 1, coarsest, forcing, corr, 0)

    @pl.when(conj(pos < last, cluster == 0))
    def _():
        corr[...] = state[...]

    pl.when(conj(pos < last, cluster > 0))(lambda: from_previous(dbuf, D, corr))

    onward = conj(follows, jnp.logical_or(cluster > 0, pos == last))
    onto_next(corr, dbuf, D, onward)
    edges(corr.at[1 : 1 + h], sbuf, (SLO, SHI), GROUP, 1, leaps)
    whole(corr.at[1 : 1 + h], sbuf, SC, GROUP, 1, leaps)
    cor_ref[...] = corr[1 : 1 + h]

    @pl.when(conj(pos == last, cluster > 0))
    def _():
        copy(held.at[0], dbuf.at[F - 1 : F + 1 + h], DC, 0, 0).wait_recv()
    outer_rows(lbuf, LLO, LHI, F - 1, odd)
    outer_rows(dbuf, DLO, DHI, F - 1, conj(odd, cluster > 0))
    outer_rows(lbuf, LOL, LOH, F - 2, conj(even, pos > 0))
    outer_rows(dbuf, DOL, DOH, F - 2, conj(even, cluster > 0))

    @pl.when(t == 0)
    def _():
        begin_ref[...] = bbuf[1 : 1 + h + 2 * F]
    @pl.when(t > 0)
    def _():
        begin_ref[...] = bufs[jnp.where(cluster > 0, 1, 0)]

    for allowed, move in sends:
        pl.when(allowed)(move.wait_send)


def relax(n_g, h, begin, cor, vel, cor_ref, rel_ref, work):
    g = lax.axis_index("gy")
    up, down = g < n_g - 1, g > 0
    F = FINE
    tiles = cor_ref.shape[-1] // LANES
    for c in range(3):
        for k in range(tiles):
            cor_ref[0, c, :, k * LANES : (k + 1) * LANES] = cor[:, c, k, :]
    here = begin
    for section in range(F):
        halo = F - section - 1
        target = work.at[section % 2]
        row = -halo
        while row < h + halo:
            size = min(BLOCK, h + halo - row)
            new = step_rows(here, F + row, vel, F + row, size, time_step)
            for c in range(3):
                for i in range(size):
                    value = new[c][i]
                    if row + i < 0:
                        value = jnp.where(down, value, 0.0)
                    elif row + i >= h:
                        value = jnp.where(up, value, 0.0)
                    target[F + row + i, c] = value
            row += size
        here = target
    for c in range(3):
        for k in range(tiles):
            rel_ref[0, c, :, k * LANES : (k + 1) * LANES] = here[F : F + h, c, k, :]


def solution(mesh):
    n_t, n_g = mesh.shape["tm"], mesh.shape["gy"]

    def per_device(initial_state, guessed_ends, velocity):
        _, h, nx = initial_state.shape
        sub = nx // LANES
        F = FINE
        out = jax.ShapeDtypeStruct(guessed_ends.shape, jnp.float32)
        f32 = lambda *shape: pltpu.VMEM(shape + (sub, LANES), jnp.float32)
        whole = pl.BlockSpec(memory_space=pltpu.VMEM)
        shape = lambda *dims: jax.ShapeDtypeStruct(dims + (sub, LANES), jnp.float32)
        begin, corrected, flow = pl.pallas_call(
            functools.partial(cycle, n_t, n_g, h),
            out_shape=(shape(h + 2 * F, 3), shape(h, 3), shape(h + 2 * F, 2)),
            in_specs=[whole] * 3,
            out_specs=(whole,) * 3,
            scratch_shapes=[
                f32(h, 3), f32(h, 3), f32(h + 2 * F + 2, 3), f32(2, h + 2 * F, 3),
                f32(2, h + 2, 3), f32(2, h + 2 * F + 2, 3), f32(4, h + 2, 3),
                pltpu.SemaphoreType.DMA((SENDS,)), pltpu.SemaphoreType.DMA((KINDS,)),
            ],
            compiler_params=pltpu.CompilerParams(
                collective_id=0, has_side_effects=True, vmem_limit_bytes=16 * 2**20),
            name="cycle",
        )(initial_state, guessed_ends, velocity)
        return pl.pallas_call(
            functools.partial(relax, n_g, h),
            out_shape=(out, out),
            in_specs=[whole] * 3,
            out_specs=(whole, whole),
            scratch_shapes=[f32(2, h + 2 * F, 3)],
            compiler_params=pltpu.CompilerParams(vmem_limit_bytes=16 * 2**20),
            name="relax",
        )(begin, corrected, flow)

    across = P("tm", None, "gy", None)
    return jax.shard_map(
        per_device, mesh=mesh, in_specs=(P(None, "gy", None), across, across),
        out_specs=(across, across), check_vma=False)
```
